16 devices in a mesh: dp: 4 (over y, z, core), tp: 4 (over x).
Axes of the slice: x: 4, y: 2, z: 1, core: 2. Of those that a mesh axis runs over, the one named last changes fastest.
The devices are a block of a 4x4x8 slice.
Arguments:
- x: bfloat16 [5632, 3072], P(('dp', 'tp')), parts along dimension 0
- w_gate: bfloat16 [3072, 8192], P(None, 'tp')
- w_up: bfloat16 [3072, 8192], P(None, 'tp')
- w_down: bfloat16 [8192, 3072], P('tp')
Outputs:
- output: bfloat16 [5632, 3072], P(('dp', 'tp')), parts along dimension 0
There are 4 independent parts. The reference program is written for one: setup_inputs(seed, part) draws one part's arguments, and reference() takes and returns one part's arrays. A program takes and returns all parts, laid end to end along the dimension named above; an argument that names none is the same for every part.
All inputs are finite; a program needn't handle non-finite values.
Results may differ from the reference program's by a relative error of at most 0.016.
Values are sent between devices in bfloat16 or wider.
A program may use at most 768 MiB of HBM per device.

```python
import jax
import jax.numpy as jnp

ROWS = 1408
D = 3072
FF = 8192


def setup_inputs(seed: int = 0, part: int = 0) -> dict:
    kx, kg, ku, kd = jax.random.split(jax.random.key(seed), 4)
    drawn = {
        "x": jax.random.normal(jax.random.fold_in(kx, part), (ROWS, D), jnp.float32),
        "w_gate": jax.random.normal(kg, (D, FF), jnp.float32) * D**-0.5,
        "w_up": jax.random.normal(ku, (D, FF), jnp.float32) * D**-0.5,
        "w_down": jax.random.normal(kd, (FF, D), jnp.float32) * FF**-0.5,
    }
    return {k: v.astype(jnp.bfloat16) for k, v in drawn.items()}


def reference(x, w_gate, w_up, w_down):
    gate = jnp.dot(x, w_gate, preferred_element_type=jnp.float32)
    up = jnp.dot(x, w_up, preferred_element_type=jnp.float32)
    hidden = (jax.nn.silu(gate) * up).astype(jnp.bfloat16)
    return jnp.dot(hidden, w_down, preferred_element_type=jnp.float32).astype(jnp.bfloat16)
```

```python
import functools

import jax
import jax.numpy as jnp
from jax import lax
from jax.experimental import pallas as pl
from jax.experimental.pallas import tpu as pltpu
from jax.sharding import PartitionSpec as P

MESH = pl.DeviceIdType.MESH
FF_TILE = 256
OUT_TILE = 512


def kernel(
    n, x_ref, wg_ref, wu_ref, wd_ref, y_ref,
    xg, vg, vu, vd, acc, hid, hid2, r_dir, r_hop, r_run,
    x_sem, wgu_sem, wd_sem, y_sem, ag_send, ag_recv, rs_send, rs_recv,
):
    rows, d = x_ref.shape
    ff = vg.shape[1]
    half = rows // 2
    n_ff, n_out = ff // FF_TILE, d // OUT_TILE
    me = lax.axis_index("tp")
    right, left = lax.rem(me + 1, n), lax.rem(me + n - 1, n)
    first, second = pl.ds(0, half), pl.ds(half, half)

    barrier = pltpu.get_barrier_semaphore()
    for neighbour in (left, right):
        pl.semaphore_signal(barrier, inc=1, device_id={"tp": neighbour}, device_id_type=MESH)

    def ff_cols(j):
        return pl.ds(pl.multiple_of(j * FF_TILE, FF_TILE), FF_TILE)

    def out_cols(j):
        return pl.ds(pl.multiple_of(j * OUT_TILE, OUT_TILE), OUT_TILE)

    def load_gate(j):
        return pltpu.make_async_copy(wg_ref.at[:, ff_cols(j)], vg.at[:, ff_cols(j)], wgu_sem.at[0, j])

    def load_up(j):
        return pltpu.make_async_copy(wu_ref.at[:, ff_cols(j)], vu.at[:, ff_cols(j)], wgu_sem.at[1, j])

    def load_down(j):
        return pltpu.make_async_copy(wd_ref.at[:, out_cols(j)], vd.at[:, out_cols(j)], wd_sem.at[j])

    load_x = pltpu.make_async_copy(x_ref, xg.at[0], x_sem)
    load_x.start()

    @pl.loop(0, n_ff)
    def _(j):
        load_gate(j).start()
        load_up(j).start()

    @pl.loop(0, n_out)
    def _(j):
        load_down(j).start()

    def remote(src, dst, sends, recvs, i, to):
        return pltpu.make_async_remote_copy(
            src_ref=src, dst_ref=dst, send_sem=sends.at[i], recv_sem=recvs.at[i],
            device_id={"tp": to}, device_id_type=MESH,
        )

    own = [
        remote(x_ref.at[first], xg.at[1, first], ag_send, ag_recv, 0, right),
        remote(x_ref.at[second], xg.at[1, second], ag_send, ag_recv, 1, left),
        remote(x_ref.at[second], xg.at[2, first], ag_send, ag_recv, 2, right),
        remote(x_ref.at[first], xg.at[2, second], ag_send, ag_recv, 3, left),
    ]
    forward = [
        remote(xg.at[1, first], xg.at[3, first], ag_send, ag_recv, 4, right),
        remote(xg.at[1, second], xg.at[3, second], ag_send, ag_recv, 5, left),
    ]

    def tile_send(src, src_half, dst, dst_half, kind, j, to):
        return pltpu.make_async_remote_copy(
            src_ref=src.at[src_half, out_cols(j)], dst_ref=dst.at[dst_half, out_cols(j)],
            send_sem=rs_send.at[kind, j], recv_sem=rs_recv.at[kind, j],
            device_id={"tp": to}, device_id_type=MESH,
        )

    def direct(j):
        return (tile_send(xg.at[0], first, r_dir, first, 0, j, left),
                tile_send(xg.at[0], second, r_dir, second, 1, j, right))

    def hop(j):
        return (tile_send(xg.at[3], second, r_hop, first, 2, j, left),
                tile_send(xg.at[3], first, r_hop, second, 3, j, right))

    def running(j):
        return (tile_send(xg.at[2], first, r_run, second, 4, j, left),
                tile_send(xg.at[2], second, r_run, first, 5, j, right))

    def start(copies):
        for copy in copies:
            copy.start()

    def recv(copies):
        for copy in copies:
            copy.wait_recv()

    def sent(copies):
        for copy in copies:
            copy.wait_send()

    pl.semaphore_wait(barrier, 2)
    start(own)

    def hidden(group, out, loading):
        @pl.loop(0, n_ff)
        def _(j):
            if loading:
                load_gate(j).wait()
                load_up(j).wait()
            gate = jnp.dot(xg[group], vg[:, ff_cols(j)], preferred_element_type=jnp.float32)
            up = jnp.dot(xg[group], vu[:, ff_cols(j)], preferred_element_type=jnp.float32)
            out[:, ff_cols(j)] = (jax.nn.silu(gate) * up).astype(out.dtype)

    def down(src, j):
        return jnp.dot(src[...], vd[:, out_cols(j)], preferred_element_type=jnp.float32)

    load_x.wait()
    hidden(0, hid, True)

    @pl.loop(0, n_out)
    def _(j):
        load_down(j).wait()
        acc[:, out_cols(j)] = down(hid, j)

    recv(own[:2])
    start(forward)
    hidden(1, hid, False)

    @pl.loop(0, n_out)
    def _(j):
        xg[0, :, out_cols(j)] = down(hid, j).astype(xg.dtype)

        @pl.when(j > 0)
        def _():
            start(direct(j - 1))

    recv(own[2:])
    start(direct(n_out - 1))
    hidden(2, hid2, False)

    recv(forward)
    hidden(3, hid, False)

    @pl.loop(0, n_out)
    def _(j):
        xg[3, :, out_cols(j)] = down(hid, j).astype(xg.dtype)

        @pl.when(j > 0)
        def _():
            start(hop(j - 1))

    recv(direct(0))
    start(hop(n_out - 1))

    @pl.loop(0, n_out)
    def _(j):
        @pl.when(j > 0)
        def _():
            recv(direct(j))

        acc[:, out_cols(j)] = acc[:, out_cols(j)] + r_dir[:, out_cols(j)].astype(jnp.float32)

    @pl.loop(0, n_out)
    def _(j):
        recv(hop(j))
        total = down(hid2, j) + r_hop[:, out_cols(j)].astype(jnp.float32)
        xg[2, :, out_cols(j)] = total.astype(xg.dtype)

        @pl.when(j > 0)
        def _():
            start(running(j - 1))

    sent(forward)
    start(running(n_out - 1))

    def store(j):
        return pltpu.make_async_copy(xg.at[1, :, out_cols(j)], y_ref.at[:, out_cols(j)], y_sem.at[j])

    @pl.loop(0, n_out)
    def _(j):
        recv(running(j))
        total = acc[:, out_cols(j)] + r_run[:, out_cols(j)].astype(jnp.float32)
        xg[1, :, out_cols(j)] = total.astype(xg.dtype)
        store(j).start()

    sent(own)

    @pl.loop(0, n_out)
    def _(j):
        sent(direct(j))
        sent(hop(j))
        sent(running(j))
        store(j).wait()


def solution(mesh):
    n = mesh.shape["tp"]

    def step(x, w_gate, w_up, w_down):
        rows, d = x.shape
        ff = w_gate.shape[1]
        n_ff, n_out = ff // FF_TILE, d // OUT_TILE
        bf16, f32 = jnp.bfloat16, jnp.float32
        block = pltpu.VMEM((rows, d), bf16)
        sem = pltpu.SemaphoreType.DMA
        return pl.pallas_call(
            functools.partial(kernel, n),
            out_shape=jax.ShapeDtypeStruct((rows, d), x.dtype),
            in_specs=[pl.BlockSpec(memory_space=pl.ANY)] * 4,
            out_specs=pl.BlockSpec(memory_space=pl.ANY),
            scratch_shapes=[
                pltpu.VMEM((4, rows, d), bf16),
                pltpu.VMEM((d, ff), bf16), pltpu.VMEM((d, ff), bf16), pltpu.VMEM((ff, d), bf16),
                pltpu.VMEM((rows, d), f32),
                pltpu.VMEM((rows, ff), bf16), pltpu.VMEM((rows, ff), bf16),
                block, block, block,
                sem, sem((2, n_ff)), sem((n_out,)), sem((n_out,)),
                sem((6,)), sem((6,)), sem((6, n_out)), sem((6, n_out)),
            ],
            compiler_params=pltpu.CompilerParams(
                collective_id=0, has_side_effects=True, vmem_limit_bytes=67_043_328
            ),
        )(x, w_gate, w_up, w_down)

    return jax.shard_map(
        step,
        mesh=mesh,
        in_specs=(P(("dp", "tp"), None), P(None, "tp"), P(None, "tp"), P("tp", None)),
        out_specs=P(("dp", "tp"), None),
        check_vma=False,
    )
```

```python
import functools

import jax
import jax.numpy as jnp
from jax import lax
from jax.experimental import pallas as pl
from jax.experimental.pallas import tpu as pltpu
from jax.sharding import PartitionSpec as P

MESH = pl.DeviceIdType.MESH
FF_TILE = 256
OUT_TILE = 512


def kernel(
    n, x_ref, wg_ref, wu_ref, wd_ref, y_ref,
    xg, vg, vu, vd, acc, hid, hid2, r_dir, r_hop, r_run,
    x_sem, wgu_sem, wd_sem, ag_send, ag_recv, rs_send, dir_recv, hop_recv, run_recv,
):
    rows, d = x_ref.shape
    ff = vg.shape[1]
    half = rows // 2
    n_ff, n_out = ff // FF_TILE, d // OUT_TILE
    me = lax.axis_index("tp")
    right, left = lax.rem(me + 1, n), lax.rem(me + n - 1, n)
    first, second = pl.ds(0, half), pl.ds(half, half)

    barrier = pltpu.get_barrier_semaphore()
    for neighbour in (left, right):
        pl.semaphore_signal(barrier, inc=1, device_id={"tp": neighbour}, device_id_type=MESH)

    def ff_cols(j):
        return pl.ds(pl.multiple_of(j * FF_TILE, FF_TILE), FF_TILE)

    def out_cols(j):
        return pl.ds(pl.multiple_of(j * OUT_TILE, OUT_TILE), OUT_TILE)

    load_x = pltpu.make_async_copy(x_ref, xg.at[0], x_sem)
    load_x.start()

    @pl.loop(0, n_ff)
    def _(j):
        pltpu.make_async_copy(wg_ref.at[:, ff_cols(j)], vg.at[:, ff_cols(j)], wgu_sem.at[j]).start()
        pltpu.make_async_copy(wu_ref.at[:, ff_cols(j)], vu.at[:, ff_cols(j)], wgu_sem.at[j]).start()

    load_down = pltpu.make_async_copy(wd_ref, vd, wd_sem)
    load_down.start()

    def remote(src, dst, send_sem, recv_sem, to):
        return pltpu.make_async_remote_copy(
            src_ref=src, dst_ref=dst, send_sem=send_sem, recv_sem=recv_sem,
            device_id={"tp": to}, device_id_type=MESH,
        )

    def wait_recv(block, sem):
        pltpu.make_async_copy(block, block, sem).wait()

    def wait_sent(block, sem):
        pltpu.make_async_copy(block, block, sem).wait()

    def gather_own():
        remote(x_ref.at[first], xg.at[1, first], ag_send, ag_recv.at[0], right).start()
        remote(x_ref.at[second], xg.at[1, second], ag_send, ag_recv.at[0], left).start()
        remote(x_ref.at[second], xg.at[2, first], ag_send, ag_recv.at[1], right).start()
        remote(x_ref.at[first], xg.at[2, second], ag_send, ag_recv.at[1], left).start()

    def gather_forward():
        remote(xg.at[1, first], xg.at[3, first], ag_send, ag_recv.at[2], right).start()
        remote(xg.at[1, second], xg.at[3, second], ag_send, ag_recv.at[2], left).start()

    def reduce_send(src, to_left, to_right, dst, at_left, at_right, sem, cols):
        remote(src.at[to_left, cols], dst.at[at_left, cols], rs_send, sem, left).start()
        remote(src.at[to_right, cols], dst.at[at_right, cols], rs_send, sem, right).start()

    def direct(j):
        reduce_send(xg.at[0], first, second, r_dir, first, second, dir_recv, out_cols(j))

    def hop(j):
        reduce_send(xg.at[3], second, first, r_hop, first, second, hop_recv.at[j], out_cols(j))

    def running(j):
        reduce_send(xg.at[2], first, second, r_run, second, first, run_recv.at[j], out_cols(j))

    pl.semaphore_wait(barrier, 2)
    gather_own()

    def hidden(group, out, loading):
        @pl.loop(0, n_ff)
        def _(j):
            if loading:
                both = pl.ds(0, 2 * FF_TILE)
                pltpu.make_async_copy(wg_ref.at[:, both], vg.at[:, both], wgu_sem.at[j]).wait()
            gate = jnp.dot(xg[group], vg[:, ff_cols(j)], preferred_element_type=jnp.float32)
            up = jnp.dot(xg[group], vu[:, ff_cols(j)], preferred_element_type=jnp.float32)
            out[:, ff_cols(j)] = (jax.nn.silu(gate) * up).astype(out.dtype)

    def down(src, j):
        return jnp.dot(src[...], vd[:, out_cols(j)], preferred_element_type=jnp.float32)

    load_x.wait()
    hidden(0, hid, True)
    load_down.wait()

    @pl.loop(0, n_out)
    def _(j):
        acc[:, out_cols(j)] = down(hid, j)

    wait_recv(xg.at[1], ag_recv.at[0])
    gather_forward()
    hidden(1, hid, False)

    @pl.loop(0, n_out)
    def _(j):
        xg[0, :, out_cols(j)] = down(hid, j).astype(xg.dtype)

        @pl.when(j > 0)
        def _():
            direct(j - 1)

    wait_recv(xg.at[2], ag_recv.at[1])
    direct(n_out - 1)
    hidden(2, hid2, False)

    wait_recv(xg.at[3], ag_recv.at[2])
    hidden(3, hid, False)

    @pl.loop(0, n_out)
    def _(j):
        xg[3, :, out_cols(j)] = down(hid, j).astype(xg.dtype)

        @pl.when(j > 0)
        def _():
            hop(j - 1)

    wait_recv(r_dir, dir_recv)
    hop(n_out - 1)

    @pl.loop(0, n_out)
    def _(j):
        acc[:, out_cols(j)] = acc[:, out_cols(j)] + r_dir[:, out_cols(j)].astype(jnp.float32)

    @pl.loop(0, n_out)
    def _(j):
        wait_recv(r_hop.at[:, out_cols(j)], hop_recv.at[j])
        total = down(hid2, j) + r_hop[:, out_cols(j)].astype(jnp.float32)
        xg[2, :, out_cols(j)] = total.astype(xg.dtype)

        @pl.when(j > 0)
        def _():
            running(j - 1)

    wait_sent(xg.at[pl.ds(0, 3)], ag_send)
    running(n_out - 1)

    @pl.loop(0, n_out)
    def _(j):
        wait_recv(r_run.at[:, out_cols(j)], run_recv.at[j])
        total = acc[:, out_cols(j)] + r_run[:, out_cols(j)].astype(jnp.float32)
        y_ref[:, out_cols(j)] = total.astype(y_ref.dtype)

    wait_sent(xg.at[pl.ds(0, 3)], rs_send)


def solution(mesh):
    n = mesh.shape["tp"]

    def step(x, w_gate, w_up, w_down):
        rows, d = x.shape
        ff = w_gate.shape[1]
        n_ff, n_out = ff // FF_TILE, d // OUT_TILE
        bf16, f32 = jnp.bfloat16, jnp.float32
        block = pltpu.VMEM((rows, d), bf16)
        sem = pltpu.SemaphoreType.DMA
        return pl.pallas_call(
            functools.partial(kernel, n),
            out_shape=pltpu.VMEM((rows, d), bf16),
            in_specs=[pl.BlockSpec(memory_space=pl.ANY)] * 4,
            out_specs=pl.BlockSpec(memory_space=pltpu.VMEM),
            scratch_shapes=[
                pltpu.VMEM((4, rows, d), bf16),
                pltpu.VMEM((d, ff), bf16), pltpu.VMEM((d, ff), bf16), pltpu.VMEM((ff, d), bf16),
                pltpu.VMEM((rows, d), f32),
                pltpu.VMEM((rows, ff), bf16), pltpu.VMEM((rows, ff), bf16),
                block, block, block,
                sem, sem((n_ff,)), sem, sem, sem((3,)), sem, sem, sem((n_out,)), sem((n_out,)),
            ],
            compiler_params=pltpu.CompilerParams(
                collective_id=0, has_side_effects=True, vmem_limit_bytes=58 * 2**20
            ),
        )(x, w_gate, w_up, w_down)

    return jax.shard_map(
        step,
        mesh=mesh,
        in_specs=(P(("dp", "tp"), None), P(None, "tp"), P(None, "tp"), P("tp", None)),
        out_specs=P(("dp", "tp"), None),
        check_vma=False,
    )
```

```python
import functools

import jax
import jax.numpy as jnp
from jax import lax
from jax.experimental import pallas as pl
from jax.experimental.pallas import tpu as pltpu
from jax.sharding import PartitionSpec as P

MESH = pl.DeviceIdType.MESH
FF_TILE = 256
OUT_TILE = 512
LAST = 256
X, R_DIR, R_HOP, R_RUN = 0, 4, 5, 6


def kernel(
    n, x_ref, wg_ref, wu_ref, wd_ref, y_ref,
    blocks, vgu, vd, acc, hid, hid2,
    x_sem, wgu_sem, wd_sem, send_sem, ag_recv, dir_recv, hop_recv, run_recv,
):
    rows, d = x_ref.shape
    ff = wg_ref.shape[1]
    half = rows // 2
    n_ff, n_out = ff // FF_TILE, d // OUT_TILE
    me = lax.axis_index("tp")
    right, left = lax.rem(me + 1, n), lax.rem(me + n - 1, n)
    first, second = pl.ds(0, half), pl.ds(half, half)
    xg = [blocks.at[X + i] for i in range(4)]
    r_dir, r_hop, r_run = blocks.at[R_DIR], blocks.at[R_HOP], blocks.at[R_RUN]

    barrier = pltpu.get_barrier_semaphore()
    for neighbour in (left, right):
        pl.semaphore_signal(barrier, inc=1, device_id={"tp": neighbour}, device_id_type=MESH)

    def ff_cols(j):
        return pl.ds(pl.multiple_of(j * FF_TILE, FF_TILE), FF_TILE)

    def out_cols(j):
        return pl.ds(pl.multiple_of(j * OUT_TILE, OUT_TILE), OUT_TILE)

    def wait(block, sem):
        pltpu.make_async_copy(block, block, sem).wait()

    pltpu.make_async_copy(x_ref, xg[0], x_sem).start()
    pltpu.make_async_copy(wg_ref, vgu.at[0], wgu_sem).start()
    pltpu.make_async_copy(wu_ref, vgu.at[1], wgu_sem).start()
    pltpu.make_async_copy(wd_ref, vd, wd_sem).start()

    def remote(src, dst, recv_sem, to):
        pltpu.make_async_remote_copy(
            src_ref=src, dst_ref=dst, send_sem=send_sem, recv_sem=recv_sem,
            device_id={"tp": to}, device_id_type=MESH,
        ).start()

    def gather_own():
        remote(x_ref.at[first], xg[1].at[first], ag_recv.at[0], right)
        remote(x_ref.at[second], xg[1].at[second], ag_recv.at[0], left)
        remote(x_ref.at[second], xg[2].at[first], ag_recv.at[1], right)
        remote(x_ref.at[first], xg[2].at[second], ag_recv.at[1], left)

    def gather_forward():
        remote(xg[1].at[first], xg[3].at[first], ag_recv.at[2], right)
        remote(xg[1].at[second], xg[3].at[second], ag_recv.at[2], left)

    def direct(j):
        cols = out_cols(j)
        remote(xg[0].at[first, cols], r_dir.at[first, cols], dir_recv, left)
        remote(xg[0].at[second, cols], r_dir.at[second, cols], dir_recv, right)

    def hop(j):
        cols = out_cols(j)
        remote(xg[3].at[second, cols], r_hop.at[first, cols], hop_recv.at[j // 2], left)
        remote(xg[3].at[first, cols], r_hop.at[second, cols], hop_recv.at[j // 2], right)

    def running(cols, piece):
        remote(xg[2].at[first, cols], r_run.at[second, cols], run_recv.at[piece], left)
        remote(xg[2].at[second, cols], r_run.at[first, cols], run_recv.at[piece], right)

    pl.semaphore_wait(barrier, 2)
    gather_own()

    def hidden(group, out):
        @pl.loop(0, n_ff)
        def _(j):
            gate = jnp.dot(xg[group][...], vgu[0, :, ff_cols(j)], preferred_element_type=jnp.float32)
            up = jnp.dot(xg[group][...], vgu[1, :, ff_cols(j)], preferred_element_type=jnp.float32)
            out[:, ff_cols(j)] = (jax.nn.silu(gate) * up).astype(out.dtype)

    def down(src, j):
        return jnp.dot(src[...], vd[:, out_cols(j)], preferred_element_type=jnp.float32)

    wait(xg[0], x_sem)
    wait(vgu, wgu_sem)
    hidden(0, hid)
    wait(vd, wd_sem)

    @pl.loop(0, n_out)
    def _(j):
        acc[:, out_cols(j)] = down(hid, j)

    wait(xg[1], ag_recv.at[0])
    gather_forward()
    hidden(1, hid)

    @pl.loop(0, n_out)
    def _(j):
        xg[0][:, out_cols(j)] = down(hid, j).astype(blocks.dtype)

        @pl.when(j > 0)
        def _():
            direct(j - 1)

    wait(xg[2], ag_recv.at[1])
    direct(n_out - 1)
    hidden(2, hid2)

    wait(xg[3], ag_recv.at[2])
    hidden(3, hid)

    @pl.loop(0, n_out)
    def _(j):
        xg[3][:, out_cols(j)] = down(hid, j).astype(blocks.dtype)

        @pl.when(j > 0)
        def _():
            hop(j - 1)

    wait(r_dir, dir_recv)
    hop(n_out - 1)

    @pl.loop(0, n_out)
    def _(j):
        acc[:, out_cols(j)] = acc[:, out_cols(j)] + r_dir[:, out_cols(j)].astype(jnp.float32)

    @pl.loop(0, n_out)
    def _(j):
        @pl.when(lax.rem(j, 2) == 0)
        def _():
            both = pl.ds(pl.multiple_of(j * OUT_TILE, 2 * OUT_TILE), 2 * OUT_TILE)
            wait(r_hop.at[:, both], hop_recv.at[j // 2])

        total = down(hid2, j) + r_hop[:, out_cols(j)].astype(jnp.float32)
        xg[2][:, out_cols(j)] = total.astype(blocks.dtype)

        @pl.when(j > 0)
        def _():
            running(out_cols(j - 1), 0)

    running(pl.ds(d - OUT_TILE, OUT_TILE - LAST), 0)
    running(pl.ds(d - LAST, LAST), 1)

    def finish(cols):
        total = acc[:, cols] + r_run[:, cols].astype(jnp.float32)
        y_ref[:, cols] = total.astype(y_ref.dtype)

    early, last = pl.ds(0, d - LAST), pl.ds(d - LAST, LAST)
    wait(r_run.at[:, early], run_recv.at[0])

    @pl.loop(0, (d - LAST) // LAST)
    def _(j):
        finish(pl.ds(pl.multiple_of(j * LAST, LAST), LAST))

    wait(blocks.at[pl.ds(0, 6)], send_sem)
    wait(r_run.at[:, last], run_recv.at[1])
    finish(last)


def solution(mesh):
    n = mesh.shape["tp"]

    def step(x, w_gate, w_up, w_down):
        rows, d = x.shape
        ff = w_gate.shape[1]
        bf16, f32 = jnp.bfloat16, jnp.float32
        sem = pltpu.SemaphoreType.DMA
        return pl.pallas_call(
            functools.partial(kernel, n),
            out_shape=pltpu.VMEM((rows, d), bf16),
            in_specs=[pl.BlockSpec(memory_space=pl.ANY)] * 4,
            out_specs=pl.BlockSpec(memory_space=pltpu.VMEM),
            scratch_shapes=[
                pltpu.VMEM((7, rows, d), bf16),
                pltpu.VMEM((2, d, ff), bf16), pltpu.VMEM((ff, d), bf16),
                pltpu.VMEM((rows, d), f32),
                pltpu.VMEM((rows, ff), bf16), pltpu.VMEM((rows, ff), bf16),
                sem, sem, sem, sem, sem((3,)), sem, sem((d // OUT_TILE // 2,)), sem((2,)),
            ],
            compiler_params=pltpu.CompilerParams(
                collective_id=0, has_side_effects=True, vmem_limit_bytes=58 * 2**20
            ),
        )(x, w_gate, w_up, w_down)

    return jax.shard_map(
        step,
        mesh=mesh,
        in_specs=(P(("dp", "tp"), None), P(None, "tp"), P(None, "tp"), P("tp", None)),
        out_specs=P(("dp", "tp"), None),
        check_vma=False,
    )
```

```python
import functools

import jax
import jax.numpy as jnp
from jax import lax
from jax.experimental import pallas as pl
from jax.experimental.pallas import tpu as pltpu
from jax.sharding import PartitionSpec as P

MESH = pl.DeviceIdType.MESH
FF_TILE = 256
OUT_TILE = 512
LAST = 256
X, R_DIR, R_HOP, R_RUN = 0, 4, 5, 6


def kernel(
    n, x_ref, wg_ref, wu_ref, wd_ref, y_ref,
    blocks, vgu, vd, acc, hid, hid2,
    x_sem, wgu_sem, wd_sem, send_sem, ag_recv, dir_recv, hop_recv, run_recv, here_sem,
):
    rows, d = x_ref.shape
    ff = wg_ref.shape[1]
    half = rows // 2
    n_ff, n_out = ff // FF_TILE, d // OUT_TILE
    me = lax.axis_index("tp")
    right, left = lax.rem(me + 1, n), lax.rem(me + n - 1, n)
    first, second = pl.ds(0, half), pl.ds(half, half)
    xg = [blocks.at[X + i] for i in range(4)]
    r_dir, r_hop, r_run = blocks.at[R_DIR], blocks.at[R_HOP], blocks.at[R_RUN]

    barrier = pltpu.get_barrier_semaphore()
    pl.semaphore_signal(barrier, inc=1, device_id={"tp": left}, device_id_type=MESH)

    def ff_cols(j):
        return pl.ds(pl.multiple_of(j * FF_TILE, FF_TILE), FF_TILE)

    def out_cols(j):
        return pl.ds(pl.multiple_of(j * OUT_TILE, OUT_TILE), OUT_TILE)

    def wait(block, sem):
        pltpu.make_async_copy(block, block, sem).wait()

    pltpu.make_async_copy(x_ref, xg[0], x_sem).start()
    pltpu.make_async_copy(wg_ref, vgu.at[0], wgu_sem).start()
    pltpu.make_async_copy(wu_ref, vgu.at[1], wgu_sem).start()
    pltpu.make_async_copy(wd_ref, vd, wd_sem).start()

    def remote(src, dst, recv_sem, to):
        pltpu.make_async_remote_copy(
            src_ref=src, dst_ref=dst, send_sem=send_sem, recv_sem=recv_sem,
            device_id={"tp": to}, device_id_type=MESH,
        ).start()

    def gather_right():
        remote(x_ref.at[first], xg[1].at[first], ag_recv.at[0], right)
        remote(x_ref.at[second], xg[2].at[first], ag_recv.at[1], right)

    def gather_left():
        remote(x_ref.at[second], xg[1].at[second], ag_recv.at[0], left)
        remote(x_ref.at[first], xg[2].at[second], ag_recv.at[1], left)

    def gather_forward():
        remote(xg[1].at[first], xg[3].at[first], ag_recv.at[2], right)
        remote(xg[1].at[second], xg[3].at[second], ag_recv.at[2], left)

    def direct(j):
        cols = out_cols(j)
        remote(xg[0].at[first, cols], r_dir.at[first, cols], dir_recv, left)
        remote(xg[0].at[second, cols], r_dir.at[second, cols], dir_recv, right)

    def hop(j):
        cols = out_cols(j)
        remote(xg[3].at[second, cols], r_hop.at[first, cols], hop_recv.at[j // 2], left)
        remote(xg[3].at[first, cols], r_hop.at[second, cols], hop_recv.at[j // 2], right)

    def running(cols, piece):
        remote(xg[2].at[first, cols], r_run.at[second, cols], run_recv.at[piece], left)
        remote(xg[2].at[second, cols], r_run.at[first, cols], run_recv.at[piece], right)

    pl.semaphore_wait(barrier, 1)
    pl.semaphore_signal(here_sem, inc=1, device_id={"tp": right}, device_id_type=MESH)
    gather_right()
    pl.semaphore_wait(here_sem, 1)
    gather_left()

    def hidden(group, out):
        @pl.loop(0, n_ff)
        def _(j):
            gate = jnp.dot(xg[group][...], vgu[0, :, ff_cols(j)], preferred_element_type=jnp.float32)
            up = jnp.dot(xg[group][...], vgu[1, :, ff_cols(j)], preferred_element_type=jnp.float32)
            out[:, ff_cols(j)] = (jax.nn.silu(gate) * up).astype(out.dtype)

    def down(src, j):
        return jnp.dot(src[...], vd[:, out_cols(j)], preferred_element_type=jnp.float32)

    wait(xg[0], x_sem)
    wait(vgu, wgu_sem)
    hidden(0, hid)
    wait(vd, wd_sem)

    @pl.loop(0, n_out)
    def _(j):
        acc[:, out_cols(j)] = down(hid, j)

    wait(xg[1], ag_recv.at[0])
    gather_forward()
    hidden(1, hid)

    @pl.loop(0, n_out)
    def _(j):
        xg[0][:, out_cols(j)] = down(hid, j).astype(blocks.dtype)

        @pl.when(j > 0)
        def _():
            direct(j - 1)

    wait(xg[2], ag_recv.at[1])
    direct(n_out - 1)
    hidden(2, hid2)

    wait(xg[3], ag_recv.at[2])
    hidden(3, hid)

    @pl.loop(0, n_out)
    def _(j):
        xg[3][:, out_cols(j)] = down(hid, j).astype(blocks.dtype)

        @pl.when(j > 0)
        def _():
            hop(j - 1)

    wait(r_dir, dir_recv)
    hop(n_out - 1)

    @pl.loop(0, n_out)
    def _(j):
        acc[:, out_cols(j)] = acc[:, out_cols(j)] + r_dir[:, out_cols(j)].astype(jnp.float32)

    @pl.loop(0, n_out)
    def _(j):
        @pl.when(lax.rem(j, 2) == 0)
        def _():
            both = pl.ds(pl.multiple_of(j * OUT_TILE, 2 * OUT_TILE), 2 * OUT_TILE)
            wait(r_hop.at[:, both], hop_recv.at[j // 2])

        total = down(hid2, j) + r_hop[:, out_cols(j)].astype(jnp.float32)
        xg[2][:, out_cols(j)] = total.astype(blocks.dtype)

        @pl.when(j > 0)
        def _():
            running(out_cols(j - 1), 0)

    running(pl.ds(d - OUT_TILE, OUT_TILE - LAST), 0)
    running(pl.ds(d - LAST, LAST), 1)

    def finish(cols):
        total = acc[:, cols] + r_run[:, cols].astype(jnp.float32)
        y_ref[:, cols] = total.astype(y_ref.dtype)

    early, last = pl.ds(0, d - LAST), pl.ds(d - LAST, LAST)
    wait(r_run.at[:, early], run_recv.at[0])

    @pl.loop(0, (d - LAST) // LAST)
    def _(j):
        finish(pl.ds(pl.multiple_of(j * LAST, LAST), LAST))

    wait(blocks.at[pl.ds(0, 6)], send_sem)
    wait(r_run.at[:, last], run_recv.at[1])
    finish(last)


def solution(mesh):
    n = mesh.shape["tp"]

    def step(x, w_gate, w_up, w_down):
        rows, d = x.shape
        ff = w_gate.shape[1]
        bf16, f32 = jnp.bfloat16, jnp.float32
        sem = pltpu.SemaphoreType.DMA
        return pl.pallas_call(
            functools.partial(kernel, n),
            out_shape=pltpu.VMEM((rows, d), bf16),
            in_specs=[pl.BlockSpec(memory_space=pl.ANY)] * 4,
            out_specs=pl.BlockSpec(memory_space=pltpu.VMEM),
            scratch_shapes=[
                pltpu.VMEM((7, rows, d), bf16),
                pltpu.VMEM((2, d, ff), bf16), pltpu.VMEM((ff, d), bf16),
                pltpu.VMEM((rows, d), f32),
                pltpu.VMEM((rows, ff), bf16), pltpu.VMEM((rows, ff), bf16),
                sem, sem, sem, sem, sem((3,)), sem, sem((d // OUT_TILE // 2,)), sem((2,)),
                pltpu.SemaphoreType.REGULAR,
            ],
            compiler_params=pltpu.CompilerParams(
                collective_id=0, has_side_effects=True, vmem_limit_bytes=58 * 2**20
            ),
        )(x, w_gate, w_up, w_down)

    return jax.shard_map(
        step,
        mesh=mesh,
        in_specs=(P(("dp", "tp"), None), P(None, "tp"), P(None, "tp"), P("tp", None)),
        out_specs=P(("dp", "tp"), None),
        check_vma=False,
    )
```

```python
import functools

import jax
import jax.numpy as jnp
from jax import lax
from jax.experimental import pallas as pl
from jax.experimental.pallas import tpu as pltpu
from jax.sharding import PartitionSpec as P

MESH = pl.DeviceIdType.MESH
FF_TILE = 256
OUT_TILE = 512
LAST = 256
X, R_DIR, R_HOP, R_RUN, S_DIR = 0, 4, 5, 6, 7


def kernel(
    n, x_ref, wg_ref, wu_ref, wd_ref, y_ref,
    blocks, vgu, vd, acc, hid, hid2,
    x_sem, wgu_sem, wd_sem, send_sem, ag_recv, dir_recv, hop_recv, run_recv, here_sem,
):
    rows, d = x_ref.shape
    ff = wg_ref.shape[1]
    half = rows // 2
    n_ff, n_out = ff // FF_TILE, d // OUT_TILE
    me = lax.axis_index("tp")
    right, left = lax.rem(me + 1, n), lax.rem(me + n - 1, n)
    first, second = pl.ds(0, half), pl.ds(half, half)
    xg = [blocks.at[X + i] for i in range(4)]
    r_dir, r_hop, r_run, s_dir = (blocks.at[i] for i in (R_DIR, R_HOP, R_RUN, S_DIR))

    barrier = pltpu.get_barrier_semaphore()
    pl.semaphore_signal(barrier, inc=1, device_id={"tp": left}, device_id_type=MESH)

    def ff_cols(j):
        return pl.ds(pl.multiple_of(j * FF_TILE, FF_TILE), FF_TILE)

    def out_cols(j):
        return pl.ds(pl.multiple_of(j * OUT_TILE, OUT_TILE), OUT_TILE)

    def wait(block, sem):
        pltpu.make_async_copy(block, block, sem).wait()

    pltpu.make_async_copy(x_ref, xg[0], x_sem).start()
    pltpu.make_async_copy(wg_ref, vgu.at[0], wgu_sem).start()
    pltpu.make_async_copy(wu_ref, vgu.at[1], wgu_sem).start()
    pltpu.make_async_copy(wd_ref, vd, wd_sem).start()

    def remote(src, dst, recv_sem, to):
        pltpu.make_async_remote_copy(
            src_ref=src, dst_ref=dst, send_sem=send_sem, recv_sem=recv_sem,
            device_id={"tp": to}, device_id_type=MESH,
        ).start()

    def gather_right():
        remote(x_ref.at[first], xg[1].at[first], ag_recv.at[0], right)
        remote(x_ref.at[second], xg[2].at[first], ag_recv.at[1], right)

    def gather_left():
        remote(x_ref.at[second], xg[1].at[second], ag_recv.at[0], left)
        remote(x_ref.at[first], xg[2].at[second], ag_recv.at[1], left)

    def gather_forward():
        remote(xg[1].at[first], xg[3].at[first], ag_recv.at[2], right)
        remote(xg[1].at[second], xg[3].at[second], ag_recv.at[2], left)

    def direct(j):
        cols = out_cols(j)
        remote(s_dir.at[first, cols], r_dir.at[first, cols], dir_recv, left)
        remote(s_dir.at[second, cols], r_dir.at[second, cols], dir_recv, right)

    def hop(j):
        cols = out_cols(j)
        remote(xg[3].at[second, cols], r_hop.at[first, cols], hop_recv.at[j // 3], left)
        remote(xg[3].at[first, cols], r_hop.at[second, cols], hop_recv.at[j // 3], right)

    def running(cols, piece):
        remote(xg[2].at[first, cols], r_run.at[second, cols], run_recv.at[piece], left)
        remote(xg[2].at[second, cols], r_run.at[first, cols], run_recv.at[piece], right)

    pl.semaphore_wait(barrier, 1)
    pl.semaphore_signal(here_sem, inc=1, device_id={"tp": right}, device_id_type=MESH)
    gather_right()
    pl.semaphore_wait(here_sem, 1)
    gather_left()

    def hidden(group, out):
        @pl.loop(0, n_ff)
        def _(j):
            gate = jnp.dot(xg[group][...], vgu[0, :, ff_cols(j)], preferred_element_type=jnp.float32)
            up = jnp.dot(xg[group][...], vgu[1, :, ff_cols(j)], preferred_element_type=jnp.float32)
            out[:, ff_cols(j)] = (jax.nn.silu(gate) * up).astype(out.dtype)

    def down(src, j):
        return jnp.dot(src[...], vd[:, out_cols(j)], preferred_element_type=jnp.float32)

    wait(xg[1], ag_recv.at[0])
    gather_forward()
    wait(vgu, wgu_sem)
    wait(vd, wd_sem)
    hidden(1, hid)

    @pl.loop(0, n_out)
    def _(j):
        s_dir[:, out_cols(j)] = down(hid, j).astype(blocks.dtype)

        @pl.when(j > 0)
        def _():
            direct(j - 1)

    wait(xg[0], x_sem)
    hidden(0, hid)
    direct(n_out - 1)

    @pl.loop(0, n_out)
    def _(j):
        acc[:, out_cols(j)] = down(hid, j)

    wait(xg[2], ag_recv.at[1])
    hidden(2, hid2)

    wait(xg[3], ag_recv.at[2])
    hidden(3, hid)

    @pl.loop(0, n_out)
    def _(j):
        xg[3][:, out_cols(j)] = down(hid, j).astype(blocks.dtype)

        @pl.when(j > 0)
        def _():
            hop(j - 1)

    wait(r_dir, dir_recv)
    hop(n_out - 1)

    @pl.loop(0, n_out)
    def _(j):
        acc[:, out_cols(j)] = acc[:, out_cols(j)] + r_dir[:, out_cols(j)].astype(jnp.float32)

    @pl.loop(0, n_out)
    def _(j):
        @pl.when(lax.rem(j, 3) == 0)
        def _():
            three = pl.ds(pl.multiple_of(j * OUT_TILE, 3 * OUT_TILE), 3 * OUT_TILE)
            wait(r_hop.at[:, three], hop_recv.at[j // 3])

        total = down(hid2, j) + r_hop[:, out_cols(j)].astype(jnp.float32)
        xg[2][:, out_cols(j)] = total.astype(blocks.dtype)

        @pl.when(j > 0)
        def _():
            running(out_cols(j - 1), 0)

    running(pl.ds(d - OUT_TILE, OUT_TILE - LAST), 0)
    running(pl.ds(d - LAST, LAST), 1)

    def finish(cols):
        total = acc[:, cols] + r_run[:, cols].astype(jnp.float32)
        y_ref[:, cols] = total.astype(y_ref.dtype)

    early, last = pl.ds(0, d - LAST), pl.ds(d - LAST, LAST)
    wait(r_run.at[:, early], run_recv.at[0])

    @pl.loop(0, (d - LAST) // LAST)
    def _(j):
        finish(pl.ds(pl.multiple_of(j * LAST, LAST), LAST))

    wait(blocks.at[pl.ds(0, 6)], send_sem)
    wait(r_run.at[:, last], run_recv.at[1])
    finish(last)


def solution(mesh):
    n = mesh.shape["tp"]

    def step(x, w_gate, w_up, w_down):
        rows, d = x.shape
        ff = w_gate.shape[1]
        bf16, f32 = jnp.bfloat16, jnp.float32
        sem = pltpu.SemaphoreType.DMA
        return pl.pallas_call(
            functools.partial(kernel, n),
            out_shape=pltpu.VMEM((rows, d), bf16),
            in_specs=[pl.BlockSpec(memory_space=pl.ANY)] * 4,
            out_specs=pl.BlockSpec(memory_space=pltpu.VMEM),
            scratch_shapes=[
                pltpu.VMEM((8, rows, d), bf16),
                pltpu.VMEM((2, d, ff), bf16), pltpu.VMEM((ff, d), bf16),
                pltpu.VMEM((rows, d), f32),
                pltpu.VMEM((rows, ff), bf16), pltpu.VMEM((rows, ff), bf16),
                sem, sem, sem, sem, sem((3,)), sem, sem((d // OUT_TILE // 3,)), sem((2,)),
                pltpu.SemaphoreType.REGULAR,
            ],
            compiler_params=pltpu.CompilerParams(
                collective_id=0, has_side_effects=True, vmem_limit_bytes=60 * 2**20
            ),
        )(x, w_gate, w_up, w_down)

    return jax.shard_map(
        step,
        mesh=mesh,
        in_specs=(P(("dp", "tp"), None), P(None, "tp"), P(None, "tp"), P("tp", None)),
        out_specs=P(("dp", "tp"), None),
        check_vma=False,
    )
```
